32 devices in a mesh: ao: 8 (over y, x, core), aux: 4 (over z).
Axes of the slice: x: 2, y: 2, z: 4, core: 2. Of those that a mesh axis runs over, the one named last changes fastest.
Arguments:
- blocks: bfloat16 [48, 256, 128, 128], P('ao', 'aux'), may hold values from -6 to 6
- pairs: int32 [48, 2], P('ao'), may hold values from 0 to 79, as said below
- counts: int32 [8], P('ao'), may hold values from 1 to 6, as said below
- owned_blocks: int32 [80], P('ao'), may hold values from 0 to 79, as said below
- occ_coef: bfloat16 [80, 8, 128], P('ao'), may hold values from -0.5 to 0.5
- vir_coef: bfloat16 [10240, 9216], P('ao', 'aux'), may hold values from -0.109375 to 0.109375
Outputs:
- b_tensor: bfloat16 [256, 8, 9216], P('ao', None, 'aux')
The draws below stay inside these ranges and needn't reach their ends.
Inputs may be any that keep to these rules, and one draw needn't show every extreme that they name: `pairs`: among the used slots of one ao index, at most 3 have nu blocks whose rows one owner holds; in every draw some index reaches 3. `counts`: some ao index uses all 6 slots in every draw. `owned_blocks`: every atom block appears exactly once.
All inputs are finite; a program needn't handle non-finite values.
Results may differ from the reference program's by a relative error of at most 0.014.
Values may be sent and summed in bfloat16 or wider, within the bound.
A program may use at most 128 MiB of HBM per device.

```python
import jax
import jax.numpy as jnp
from jax import lax

BLK = 128
BLK_DEV = 10
OCC = 8
SLOTS = 6
NBLK = 80
NAO = 10240
PS = 256
V = 9216
CAP = 3
ALL_SLOTS = 48
N_AO = 8


def slot_layout(key):
    perm_blocks = jax.random.permutation(jax.random.fold_in(key, 11), NBLK).astype(jnp.int32)
    used_counts = jax.random.randint(jax.random.fold_in(key, 12), (N_AO,), 1, SLOTS + 1).astype(jnp.int32)
    full_index = jax.random.randint(jax.random.fold_in(key, 13), (), 0, N_AO)
    used_counts = jnp.where(jnp.arange(N_AO) == full_index, SLOTS, used_counts).astype(jnp.int32)
    first_owner = jax.random.randint(jax.random.fold_in(key, 14), (N_AO,), 0, N_AO)
    second_owner = (first_owner + 1 + jax.random.randint(jax.random.fold_in(key, 15), (N_AO,), 0, N_AO - 1)) % N_AO
    slot_half = jnp.arange(SLOTS) // CAP
    owner_pick = jnp.where(slot_half[None, :] == 0, first_owner[:, None], second_owner[:, None])
    local_pick = jax.random.randint(jax.random.fold_in(key, 16), (N_AO, SLOTS), 0, BLK_DEV)
    second_block = perm_blocks[owner_pick * BLK_DEV + local_pick]
    first_block = jax.random.randint(jax.random.fold_in(key, 17), (N_AO, SLOTS), 0, NBLK)
    pair_list = jnp.stack([first_block, second_block], axis=-1).reshape(N_AO * SLOTS, 2).astype(jnp.int32)
    return (pair_list, used_counts, perm_blocks)


def draw_pairs(key, part):
    return slot_layout(key)[0]


def draw_counts(key, part):
    return slot_layout(key)[1]


def draw_owned_blocks(key, part):
    return slot_layout(key)[2]


def steps_of(stream_key, extent, shards, low, top_value):
    factor_of, own = 1.0, jax.random.fold_in(stream_key, 6)
    for axis_at, shards_of in shards:
        draws = jnp.exp(jax.random.uniform(jax.random.fold_in(own, axis_at), (shards_of,), jnp.float32, low / len(shards), top_value / len(shards)))
        factor_of = factor_of * jnp.repeat(draws, extent[axis_at] // shards_of).reshape([-1 if axis == axis_at else 1 for axis in range(len(extent))])
    return factor_of


def scatter_about(rng, shape, width, bound, pieces=(), kind=jnp.bfloat16):
    array = jax.random.normal(rng, shape, jnp.float32) * width
    if len(pieces) > 0:
        array = steps_of(rng, shape, pieces, -0.22, 0.18) * array
    return jnp.clip(array, min=-bound, max=bound).astype(kind)


def setup_inputs(seed: int = 0) -> dict:
    streams_of = jax.random.split(jax.random.key(seed), 7)
    blocks = scatter_about(streams_of[0], (ALL_SLOTS, PS, BLK, BLK), 1.0, 6.0, ((0, 8), (1, 4)))
    pairs = draw_pairs(jax.random.fold_in(streams_of[6], 71), 0)
    counts = draw_counts(jax.random.fold_in(streams_of[6], 71), 0)
    owned_blocks = draw_owned_blocks(jax.random.fold_in(streams_of[6], 71), 0)
    occ_coef = scatter_about(streams_of[4], (NBLK, OCC, BLK), BLK ** -0.5, 0.5, ((0, 8),))
    vir_coef = scatter_about(streams_of[5], (NAO, V), (BLK * ALL_SLOTS // 2) ** -0.5, 0.109375, ((0, 8), (1, 4)))
    return {"blocks": blocks, "pairs": pairs, "counts": counts, "owned_blocks": owned_blocks, "occ_coef": occ_coef, "vir_coef": vir_coef}


def half_slab(args):
    block, coef, in_use = args
    value = jnp.einsum("im,pmn->pin", coef.astype(jnp.float32), block.astype(jnp.float32))
    return jnp.where(in_use, value, jnp.zeros_like(value)).astype(jnp.bfloat16)


def reference(blocks, pairs, counts, owned_blocks, occ_coef, vir_coef):
    total_blocks = owned_blocks.shape[0]
    slot_total = pairs.shape[0]
    slot_count = slot_total // N_AO
    block_width = blocks.shape[2]
    positions = jnp.arange(total_blocks, dtype=jnp.int32)
    place = jnp.zeros((total_blocks,), jnp.int32).at[owned_blocks].set(positions)
    in_use = (jnp.arange(slot_count, dtype=jnp.int32)[None, :] < counts[:, None]).reshape(-1)
    row_first = place[pairs[:, 0]]
    row_second = place[pairs[:, 1]]
    slabs = lax.map(half_slab, (blocks, occ_coef[row_first], in_use))
    gathered = jax.ops.segment_sum(slabs.astype(jnp.float32), row_second, num_segments=total_blocks)
    gathered = gathered.astype(jnp.bfloat16)
    per_owner = total_blocks // N_AO
    occupied = occ_coef.shape[1]
    total = jnp.zeros((PS * occupied, vir_coef.shape[1]), jnp.float32)
    for owner_idx in range(N_AO):
        part = gathered[owner_idx * per_owner:(owner_idx + 1) * per_owner]
        left = jnp.transpose(part, (1, 2, 0, 3)).reshape(PS * occupied, per_owner * block_width)
        right = vir_coef[owner_idx * per_owner * block_width:(owner_idx + 1) * per_owner * block_width]
        term = jnp.dot(left, right, preferred_element_type=jnp.float32).astype(jnp.bfloat16)
        total = total + term.astype(jnp.float32)
    return total.reshape(PS, occupied, vir_coef.shape[1]).astype(jnp.bfloat16)
```

```python
import functools

import jax
import jax.numpy as jnp
from jax import lax
from jax.experimental import pallas as pl
from jax.experimental.pallas import tpu as pltpu
from jax.sharding import PartitionSpec as P

MESH = pl.DeviceIdType.MESH
CAP = 3
CHUNKS = 4


def few_blocks(per_owner):
    return -(-per_owner * 2 // 3)


def block_place(block_ids, owned_all):
    hits = block_ids[..., None] == owned_all
    positions = jnp.arange(owned_all.shape[0], dtype=jnp.int32)
    return jnp.sum(jnp.where(hits, positions, 0), axis=-1)


def small_kernel(n, meta_ref, occ_ref, meta_out, occ_out, s_sem, r_sem, l_sem):
    me = lax.axis_index("ao")
    barrier = pltpu.get_barrier_semaphore()
    for k in range(1, n):
        pl.semaphore_signal(barrier, inc=1, device_id={"ao": lax.rem(me + k, n)}, device_id_type=MESH)
    own = [
        pltpu.make_async_copy(meta_ref, meta_out.at[me], l_sem.at[0]),
        pltpu.make_async_copy(occ_ref, occ_out.at[me], l_sem.at[1]),
    ]
    for copy in own:
        copy.start()
    pl.semaphore_wait(barrier, n - 1)
    sent = []
    for k in range(1, n):
        for which, (src, dst) in enumerate(((meta_ref, meta_out), (occ_ref, occ_out))):
            copy = pltpu.make_async_remote_copy(
                src_ref=src, dst_ref=dst.at[me], send_sem=s_sem.at[which, k], recv_sem=r_sem.at[which, k],
                device_id={"ao": lax.rem(me + k, n)}, device_id_type=MESH,
            )
            copy.start()
            sent.append(copy)
    for copy in own + sent:
        copy.wait()


def gather_small(n, meta, occ):
    return pl.pallas_call(
        functools.partial(small_kernel, n),
        out_shape=(
            jax.ShapeDtypeStruct((n,) + meta.shape, meta.dtype),
            jax.ShapeDtypeStruct((n,) + occ.shape, occ.dtype),
        ),
        in_specs=[pl.BlockSpec(memory_space=pltpu.VMEM)] * 2,
        out_specs=(pl.BlockSpec(memory_space=pltpu.VMEM),) * 2,
        scratch_shapes=[
            pltpu.SemaphoreType.DMA((2, n)),
            pltpu.SemaphoreType.DMA((2, n)),
            pltpu.SemaphoreType.DMA((2,)),
        ],
        compiler_params=pltpu.CompilerParams(collective_id=0, has_side_effects=True),
    )(meta, occ)


def main_kernel(
    n, nz, kept, idx_ref, w_ref, pick_ref, half_ref, vir_hbm, out_ref,
    vir_all, vir, snd, rcv, rows, part, pair, rx, ry, tx, ty,
    vir_sem, own_sem, a_s, a_r, up_s, up_r, dn_s, dn_r, p_s, p_r, x_s, x_r, y_s, y_r,
):
    me, z = lax.axis_index("ao"), lax.axis_index("aux")
    core, chip = lax.rem(me, 2), me // 2
    cx, cy = lax.rem(chip, 2), chip // 2
    mate = me + 1 - 2 * core
    xmate = me + 2 - 4 * cx
    ymate = me + 4 - 8 * cy
    total = n * CAP
    width = rcv.shape[-1]
    step = rcv.shape[3]
    mid = step // 2

    barrier = pltpu.get_barrier_semaphore()
    for k in range(1, n):
        pl.semaphore_signal(barrier, inc=1, device_id={"ao": lax.rem(me + k, n)}, device_id_type=MESH)
    for k in range(1, nz):
        pl.semaphore_signal(barrier, inc=1, device_id={"aux": lax.rem(z + k, nz)}, device_id_type=MESH)
    vir_copy = pltpu.make_async_copy(vir_hbm, vir_all, vir_sem)
    vir_copy.start()

    def pack(i, carry):
        snd[i] = half_ref[idx_ref[i]]
        return carry

    lax.fori_loop(0, total, pack, 0)
    pl.semaphore_wait(barrier, n + nz - 2)

    a_copies = []
    for c in range(CHUNKS):
        span = pl.ds(c * step, step)
        mine = pl.ds(me * CAP, CAP)
        local = pltpu.make_async_copy(snd.at[mine, :, span, :], rcv.at[c, mine], own_sem.at[c])
        local.start()
        group = [local]
        for k in range(1, n):
            dst = lax.rem(me + k, n)
            copy = pltpu.make_async_remote_copy(
                src_ref=snd.at[pl.ds(dst * CAP, CAP), :, span, :], dst_ref=rcv.at[c, mine],
                send_sem=a_s.at[c, k], recv_sem=a_r.at[c, k],
                device_id={"ao": dst}, device_id_type=MESH,
            )
            copy.start()
            group.append(copy)
        a_copies.append(group)

    def z_copy(c, d, up):
        src = z - d if up else z + d
        return pltpu.make_async_remote_copy(
            src_ref=rows.at[c, src], dst_ref=rows.at[c, src],
            send_sem=(up_s if up else dn_s).at[c, d], recv_sem=(up_r if up else dn_r).at[c, d],
            device_id={"aux": z + 1 if up else z - 1}, device_id_type=MESH,
        )

    def z_send(c, d):
        @pl.when((z - d >= 0) & (z + 1 < nz))
        def _():
            z_copy(c, d, True).start()

        @pl.when((z + d < nz) & (z >= 1))
        def _():
            z_copy(c, d, False).start()

    def z_recv(c, d, up):
        src = z - d if up else z + d
        return pltpu.make_async_remote_copy(
            src_ref=rows.at[c, src], dst_ref=rows.at[c, src],
            send_sem=(up_s if up else dn_s).at[c, d - 1], recv_sem=(up_r if up else dn_r).at[c, d - 1],
            device_id={"aux": z - 1 if up else z + 1}, device_id_type=MESH,
        )

    def stage_a(c):
        a_copies[c][0].wait()
        for copy in a_copies[c][1:]:
            copy.wait_recv()
        for l in range(kept):
            def add(s, acc):
                for j in range(CAP):
                    t = s * CAP + j
                    acc = acc + w_ref[l * total + t] * rcv[c, t].astype(jnp.float32)
                return acc

            acc = lax.fori_loop(0, n, add, jnp.zeros((2, step, width), jnp.float32))
            rows[c, z, :, l * width:(l + 1) * width] = acc.reshape(2 * step, width).astype(jnp.bfloat16)
        z_send(c, 0)

    def stage_b(c, d):
        @pl.when(z - d >= 0)
        def _():
            z_recv(c, d, True).wait_recv()

        @pl.when(z + d < nz)
        def _():
            z_recv(c, d, False).wait_recv()

        if d < nz - 1:
            z_send(c, d)

    pair_copies, x_copies, y_copies = {}, {}, {}

    def remote(src, dst, ss, rs, to):
        copy = pltpu.make_async_remote_copy(
            src_ref=src, dst_ref=dst, send_sem=ss, recv_sem=rs, device_id={"ao": to}, device_id_type=MESH,
        )
        copy.start()
        return copy

    tile = 256
    depth = rows.shape[-1]

    def stage_m(c):
        @pl.loop(0, vir.shape[1] // tile)
        def _(j):
            cols = pl.ds(pl.multiple_of(j * tile, tile), tile)
            left = rows[c].reshape(nz * 2 * step, depth)
            got = jnp.dot(left, vir[:, cols], preferred_element_type=jnp.float32)
            got = got.astype(jnp.bfloat16).reshape(nz, 2, step, tile)
            for h in range(2):
                part[c, h, :, :, cols] = got[:, h]

        pair_copies[c] = remote(part.at[c, 1 - core], pair.at[c], p_s.at[c], p_r.at[c], mate)

    def add2(a, b):
        return (a.astype(jnp.float32) + b.astype(jnp.float32)).astype(jnp.bfloat16)

    def stage_p(c):
        pair_copies[c].wait_recv()

        @pl.loop(0, nz)
        def _(i):
            pair[c, i] = add2(pair[c, i], part[c, core, i])

        lo, hi = pl.ds(0, mid), pl.ds(mid, mid)
        x_copies[c] = [
            remote(pair.at[c, 1 - cx, lo], rx.at[c, 0], x_s.at[c, 0], x_r.at[c, 0], xmate),
            remote(pair.at[c, 2 * (1 - cy), hi], ry.at[c, 0], y_s.at[c, 0], y_r.at[c, 0], ymate),
            remote(pair.at[c, 3 - cx, lo], rx.at[c, 1], x_s.at[c, 1], x_r.at[c, 1], xmate),
            remote(pair.at[c, 2 * (1 - cy) + 1, hi], ry.at[c, 1], y_s.at[c, 1], y_r.at[c, 1], ymate),
        ]

    def stage_x(c):
        for copy in x_copies[c]:
            copy.wait_recv()
        tx[c] = add2(pair[c, 2 * (1 - cy) + cx, :mid], rx[c, 1 - cy])
        ty[c] = add2(pair[c, 2 * cy + 1 - cx, mid:], ry[c, 1 - cx])
        y_copies[c] = [
            remote(tx.at[c], rx.at[c, 2], y_s.at[c, 2], y_r.at[c, 2], ymate),
            remote(ty.at[c], ry.at[c, 2], x_s.at[c, 2], x_r.at[c, 2], xmate),
        ]

    def stage_y(c):
        for copy in y_copies[c]:
            copy.wait_recv()
        f32 = jnp.float32
        own = pair[c, 2 * cy + cx]
        top = own[:mid].astype(f32) + rx[c, cy].astype(f32) + rx[c, 2].astype(f32)
        low = own[mid:].astype(f32) + ry[c, cx].astype(f32) + ry[c, 2].astype(f32)
        out_ref[c * step:c * step + mid, :] = top.astype(jnp.bfloat16)
        out_ref[c * step + mid:(c + 1) * step, :] = low.astype(jnp.bfloat16)

    vir_copy.wait()
    piece = 16

    @pl.loop(0, width // piece)
    def _(i):
        at = pl.ds(pl.multiple_of(i * piece, piece), piece)
        for k in range(kept):
            to = pl.ds(pl.multiple_of(k * width + i * piece, piece), piece)
            vir[to, :] = vir_all[pick_ref[k], at, :]

    plan = (
        "A0 B01 A1 B02", "A2 B11 B03 M0", "A3 B12 B21 P0", "B13 M1 B22 B31",
        "X0 P1 B23 M2", "B32 Y0 X1 P2", "B33 M3 Y1 X2", "P3 Y2 X3 Y3",
    )
    run = {"A": stage_a, "B": stage_b, "M": stage_m, "P": stage_p, "X": stage_x, "Y": stage_y}
    for item in [name for row in plan for name in row.split()]:
        run[item[0]](*[int(v) for v in item[1:]])

    for c in range(CHUNKS):
        for copy in a_copies[c][1:] + [pair_copies[c]] + x_copies[c] + y_copies[c]:
            copy.wait_send()
        for d in range(nz - 1):
            @pl.when((z - d >= 0) & (z + 1 < nz))
            def _():
                z_copy(c, d, True).wait_send()

            @pl.when((z + d < nz) & (z >= 1))
            def _():
                z_copy(c, d, False).wait_send()


def fused(n, nz, kept, call_id, idx, weights, pick, half, vir_coef):
    _, _, span, width = half.shape
    step = span // CHUNKS
    columns = vir_coef.shape[2]
    bf = jnp.bfloat16
    dma = pltpu.SemaphoreType.DMA
    vm = pltpu.VMEM
    return pl.pallas_call(
        functools.partial(main_kernel, n, nz, kept),
        out_shape=jax.ShapeDtypeStruct((span, columns), bf),
        in_specs=[
            pl.BlockSpec(memory_space=pltpu.SMEM),
            pl.BlockSpec(memory_space=pltpu.SMEM),
            pl.BlockSpec(memory_space=pltpu.SMEM),
            pl.BlockSpec(memory_space=pltpu.VMEM),
            pl.BlockSpec(memory_space=pl.ANY),
        ],
        out_specs=pl.BlockSpec(memory_space=pltpu.VMEM),
        scratch_shapes=[
            vm(vir_coef.shape, bf),
            vm((kept * width, columns), bf),
            vm((n * CAP, 2, span, width), bf),
            vm((CHUNKS, n * CAP, 2, step, width), bf),
            vm((CHUNKS, nz, 2 * step, kept * width), bf),
            vm((CHUNKS, 2, nz, step, columns), bf),
            vm((CHUNKS, nz, step, columns), bf),
            vm((CHUNKS, 3, step // 2, columns), bf),
            vm((CHUNKS, 3, step // 2, columns), bf),
            vm((CHUNKS, step // 2, columns), bf),
            vm((CHUNKS, step // 2, columns), bf),
            dma, dma((CHUNKS,)),
            dma((CHUNKS, n)), dma((CHUNKS, n)),
            dma((CHUNKS, nz)), dma((CHUNKS, nz)), dma((CHUNKS, nz)), dma((CHUNKS, nz)),
            dma((CHUNKS,)), dma((CHUNKS,)),
            dma((CHUNKS, 3)), dma((CHUNKS, 3)), dma((CHUNKS, 3)), dma((CHUNKS, 3)),
        ],
        compiler_params=pltpu.CompilerParams(
            collective_id=call_id, has_side_effects=True, vmem_limit_bytes=62 * 1024 * 1024,
        ),
    )(idx, weights, pick, half, vir_coef)


def per_device(blocks, pairs, counts, owned_blocks, occ_coef, vir_coef):
    groups, nz = lax.axis_size("ao"), lax.axis_size("aux")
    me = lax.axis_index("ao")
    slots, aux_depth, _, width = blocks.shape
    per_owner, occupied, _ = occ_coef.shape
    flat = jnp.concatenate([pairs.reshape(-1), counts, owned_blocks])
    used = flat.shape[0]
    meta = jnp.broadcast_to(jnp.pad(flat, (0, -used % 128))[None], (8, used + -used % 128))
    meta_all, occ_all = gather_small(groups, meta, occ_coef.reshape(per_owner * occupied, width))
    meta_all = meta_all[:, 0]
    all_pairs = meta_all[:, :2 * slots].reshape(groups, slots, 2)
    all_counts = meta_all[:, 2 * slots]
    all_owned = meta_all[:, 2 * slots + 1:used].reshape(-1)
    occ_all = occ_all.reshape(groups * per_owner, occupied, width)

    slot_ids = jnp.arange(slots, dtype=jnp.int32)
    in_use = slot_ids < counts[0]
    occ_pick = occ_all[block_place(pairs[:, 0], all_owned)]
    half = jnp.einsum("sim,spmn->spin", occ_pick, blocks, preferred_element_type=jnp.float32)
    half = jnp.where(in_use[:, None, None, None], half, 0.0).astype(jnp.bfloat16)
    half = half.reshape(slots, 2, aux_depth * occupied // 2, width)

    place = block_place(all_pairs[:, :, 1], all_owned)
    live = slot_ids[None, :] < all_counts[:, None]
    owner, local = place // per_owner, place % per_owner
    same = (owner[:, :, None] == owner[:, None, :]) & live[:, None, :]
    rank = jnp.sum(jnp.where(same & (slot_ids[None, None, :] < slot_ids[None, :, None]), 1, 0), axis=-1)
    ranks = jnp.arange(CAP, dtype=jnp.int32)
    mine = live & (owner == me)
    positions = jnp.arange(per_owner, dtype=jnp.int32)
    hit = live[None, None] & (place[None, None] == (
        jnp.arange(groups, dtype=jnp.int32)[:, None] * per_owner + positions)[:, :, None, None])
    seen = jnp.any(hit, axis=(2, 3))
    most = jnp.max(jnp.sum(jnp.where(seen, 1, 0), axis=1))
    my_seen = jnp.any(mine[None] & (local[None] == positions[:, None, None]), axis=(1, 2))
    order = jnp.sum(jnp.where(my_seen[None, :] & (positions[None, :] < positions[:, None]), 1, 0), axis=1)
    listed = my_seen[None, :] & (order[None, :] == positions[:, None])
    pick = jnp.sum(jnp.where(listed, positions[None, :], 0), axis=1)
    spot = jnp.sum(jnp.where(local[:, :, None] == positions, order, 0), axis=-1)
    weights = (
        mine[None, :, None, :]
        & (spot[None, :, None, :] == positions[:, None, None, None])
        & (rank[None, :, None, :] == ranks[None, None, :, None])
    )
    weights = jnp.sum(jnp.where(weights, 1.0, 0.0), axis=-1).reshape(-1)
    my_owner, my_live, my_rank = (jnp.take(v, me, axis=0) for v in (owner, live, rank))
    chosen = (
        my_live[None, None, :]
        & (my_owner[None, None, :] == jnp.arange(groups, dtype=jnp.int32)[:, None, None])
        & (my_rank[None, None, :] == ranks[None, :, None])
    )
    idx = jnp.sum(jnp.where(chosen, slot_ids, 0), axis=-1).reshape(-1)
    few = few_blocks(per_owner)
    vir3 = vir_coef.reshape(per_owner, width, vir_coef.shape[1])
    out = lax.cond(
        most <= few,
        functools.partial(fused, groups, nz, few, 1),
        functools.partial(fused, groups, nz, per_owner, 2),
        idx, weights, pick, half, vir3,
    )
    return out.reshape(-1, occupied, vir_coef.shape[1])


def per_device_general(blocks, pairs, counts, owned_blocks, occ_coef, vir_coef):
    groups = lax.axis_size("ao")
    own_index = lax.axis_index("ao")
    slot_count = blocks.shape[0]
    aux_depth = blocks.shape[1]
    block_width = blocks.shape[3]
    occupied = occ_coef.shape[1]
    all_pairs, all_counts, all_owned = (
        lax.all_gather(pairs, "ao", axis=0, tiled=True),
        lax.all_gather(counts, "ao", axis=0, tiled=True),
        lax.all_gather(owned_blocks, "ao", axis=0, tiled=True),
    )
    occ_all = lax.all_gather(occ_coef, "ao", axis=0, tiled=True)
    per_owner = all_owned.shape[0] // groups
    slot_ids = jnp.arange(slot_count, dtype=jnp.int32)
    in_use = slot_ids < counts[0]
    occ_pick = occ_all[block_place(pairs[:, 0], all_owned)]
    slab_values = jnp.einsum("sim,spmn->spin", occ_pick, blocks, preferred_element_type=jnp.float32)
    slab_values = jnp.where(in_use[:, None, None, None], slab_values, 0.0).astype(jnp.bfloat16)
    flat_slabs = slab_values.reshape(slot_count, aux_depth * occupied, block_width)
    place_all = block_place(all_pairs[:, 1], all_owned).reshape(groups, slot_count)
    owner_all = place_all // per_owner
    local_all = place_all % per_owner
    live_all = slot_ids[None, :] < all_counts[:, None]
    mine_all = live_all & (owner_all == own_index)
    local_ids = jnp.arange(per_owner, dtype=jnp.int32)
    slabs_got = lax.all_gather(flat_slabs, "ao", axis=0, tiled=True)
    assign = (
        mine_all.reshape(-1)[None, :] & (local_all.reshape(-1)[None, :] == local_ids[:, None])
    ).astype(jnp.bfloat16)
    summed = jnp.einsum("lt,tqm->qlm", assign, slabs_got, preferred_element_type=jnp.float32)
    rows_local = summed.reshape(summed.shape[0], per_owner * block_width).astype(jnp.bfloat16)
    rows_whole = lax.all_gather(rows_local, "aux", axis=0, tiled=True)
    share = rows_whole.shape[0] // groups
    result = lax.psum_scatter(
        jnp.dot(rows_whole, vir_coef, preferred_element_type=jnp.float32).astype(jnp.bfloat16),
        "ao",
        scatter_dimension=0,
        tiled=True,
    )
    return result.reshape(share // occupied, occupied, vir_coef.shape[1])


def solution(mesh):
    in_specs = (
        P("ao", "aux", None, None),
        P("ao", None),
        P("ao"),
        P("ao"),
        P("ao", None, None),
        P("ao", "aux"),
    )
    out_specs = P("ao", None, "aux")
    small = mesh.shape["ao"] == 8 and mesh.shape["aux"] == 4
    body = per_device if small else per_device_general
    return jax.shard_map(body, mesh=mesh, in_specs=in_specs, out_specs=out_specs, check_vma=False)
```
